16 devices in a mesh: data: 4 (over z, y), tensor: 4 (over x, core).
Axes of the slice: x: 2, y: 2, z: 2, core: 2. Of those that a mesh axis runs over, the one named last changes fastest.
Arguments:
- x: bfloat16 [64, 1024, 1024], P('data'), parts along dimension 0
- adapter_ids: int32 [64], P('data'), parts along dimension 0
- norm_gain: float32 [1024], replicated
- w_query: bfloat16 [1024, 16, 64], P(None, 'tensor')
- w_key: bfloat16 [1024, 16, 64], P(None, 'tensor')
- w_value: bfloat16 [1024, 16, 64], P(None, 'tensor')
- w_out: bfloat16 [16, 64, 1024], P('tensor')
- w_gate: bfloat16 [1024, 4096], P(None, 'tensor')
- w_up: bfloat16 [1024, 4096], P(None, 'tensor')
- w_down: bfloat16 [4096, 1024], P('tensor')
- lora_a_query: bfloat16 [64, 1024, 16], P(None, None, 'tensor')
- lora_b_query: bfloat16 [64, 16, 16, 64], P(None, None, 'tensor')
- lora_a_key: bfloat16 [64, 1024, 16], P(None, None, 'tensor')
- lora_b_key: bfloat16 [64, 16, 16, 64], P(None, None, 'tensor')
- lora_a_value: bfloat16 [64, 1024, 16], P(None, None, 'tensor')
- lora_b_value: bfloat16 [64, 16, 16, 64], P(None, None, 'tensor')
- lora_a_out: bfloat16 [64, 16, 64, 16], P(None, 'tensor')
- lora_b_out: bfloat16 [64, 16, 1024], P(None, None, 'tensor')
- lora_a_gate: bfloat16 [64, 1024, 16], P(None, None, 'tensor')
- lora_b_gate: bfloat16 [64, 16, 4096], P(None, None, 'tensor')
- lora_a_up: bfloat16 [64, 1024, 16], P(None, None, 'tensor')
- lora_b_up: bfloat16 [64, 16, 4096], P(None, None, 'tensor')
- lora_a_down: bfloat16 [64, 4096, 16], P(None, 'tensor')
- lora_b_down: bfloat16 [64, 16, 1024], P(None, None, 'tensor')
Outputs:
- output: bfloat16 [64, 1024, 1024], P('data'), parts along dimension 0
There are 4 independent parts. The reference program is written for one: setup_inputs(seed, part) draws one part's arguments, and reference() takes and returns one part's arrays. A program takes and returns all parts, laid end to end along the dimension named above; an argument that names none is the same for every part.
All inputs are finite; a program needn't handle non-finite values.
Results may differ from the reference program's by a relative error of at most 0.012043.
Values are sent between devices in bfloat16 or wider.
A program may use at most 1 GiB of HBM per device.

```python
import jax
import jax.numpy as jnp
import math
from jax import lax

SEQS = 16
SEQLEN = 1024
D = 1024
HEADS = 16
HEAD = 64
FF = 4096
R = 16
ADAPTERS = 64
ALPHA = 16

EPS = 1e-5
ROPE_BASE = 10000.0
SCALE = ALPHA / R
LORA_FRAC = 0.2


def normal_draw(key, shape, std):
    return (jax.random.normal(key, shape, jnp.float32) * std).astype(jnp.bfloat16)


def setup_inputs(seed: int = 0, part: int = 0) -> dict:
    root = jax.random.key(seed)
    part_key = jax.random.fold_in(root, part)
    x_key, id_key, slot_key = jax.random.split(part_key, 3)
    keys = jax.random.split(root, 22)
    hid_width = HEADS * HEAD
    qk_std = math.log(SEQLEN / 16.0) ** 0.25
    b_std = LORA_FRAC * math.sqrt(R) / ALPHA
    in_std = 1.0 / math.sqrt(D)
    adapter_ids = jax.random.randint(id_key, (SEQS,), 0, ADAPTERS, dtype=jnp.int32)
    slots = jax.random.permutation(slot_key, SEQS)
    adapter_ids = adapter_ids.at[slots[0]].set(ADAPTERS - 1).at[slots[1]].set(0)
    return {
        'x': normal_draw(x_key, (SEQS, SEQLEN, D), 1.0),
        'adapter_ids': adapter_ids,
        'norm_gain': 1.0 + 0.2 * jax.random.normal(keys[0], (D,), jnp.float32),
        'w_query': normal_draw(keys[1], (D, HEADS, HEAD), qk_std * in_std),
        'w_key': normal_draw(keys[2], (D, HEADS, HEAD), qk_std * in_std),
        'w_value': normal_draw(keys[3], (D, HEADS, HEAD), in_std),
        'w_out': normal_draw(keys[4], (HEADS, HEAD, D), 1.0 / math.sqrt(hid_width)),
        'w_gate': normal_draw(keys[5], (D, FF), in_std),
        'w_up': normal_draw(keys[6], (D, FF), in_std),
        'w_down': normal_draw(keys[7], (FF, D), 1.0 / math.sqrt(FF)),
        'lora_a_query': normal_draw(keys[8], (ADAPTERS, D, R), in_std),
        'lora_b_query': normal_draw(keys[9], (ADAPTERS, R, HEADS, HEAD), qk_std * b_std),
        'lora_a_key': normal_draw(keys[10], (ADAPTERS, D, R), in_std),
        'lora_b_key': normal_draw(keys[11], (ADAPTERS, R, HEADS, HEAD), qk_std * b_std),
        'lora_a_value': normal_draw(keys[12], (ADAPTERS, D, R), in_std),
        'lora_b_value': normal_draw(keys[13], (ADAPTERS, R, HEADS, HEAD), b_std),
        'lora_a_out': normal_draw(keys[14], (ADAPTERS, HEADS, HEAD, R), 1.0 / math.sqrt(hid_width)),
        'lora_b_out': normal_draw(keys[15], (ADAPTERS, R, D), b_std),
        'lora_a_gate': normal_draw(keys[16], (ADAPTERS, D, R), in_std),
        'lora_b_gate': normal_draw(keys[17], (ADAPTERS, R, FF), b_std),
        'lora_a_up': normal_draw(keys[18], (ADAPTERS, D, R), in_std),
        'lora_b_up': normal_draw(keys[19], (ADAPTERS, R, FF), b_std),
        'lora_a_down': normal_draw(keys[20], (ADAPTERS, FF, R), 1.0 / math.sqrt(FF)),
        'lora_b_down': normal_draw(keys[21], (ADAPTERS, R, D), b_std),
    }


def rope_rotate(vals, cos_t, sin_t):
    half_dim = vals.shape[-1] // 2
    first = vals[..., :half_dim]
    second = vals[..., half_dim:]
    return jnp.concatenate([first * cos_t - second * sin_t, second * cos_t + first * sin_t], axis=-1)


def lora_proj(rows_in, weight, a_stack, b_stack, adapter):
    base_out = jnp.dot(rows_in, weight, preferred_element_type=jnp.float32)
    lora_mid = jnp.dot(rows_in, a_stack[adapter], preferred_element_type=jnp.float32).astype(jnp.bfloat16)
    return base_out + SCALE * jnp.dot(lora_mid, b_stack[adapter], preferred_element_type=jnp.float32)


def reference(x, adapter_ids, norm_gain, w_query, w_key, w_value, w_out, w_gate, w_up, w_down, lora_a_query, lora_b_query, lora_a_key, lora_b_key, lora_a_value, lora_b_value, lora_a_out, lora_b_out, lora_a_gate, lora_b_gate, lora_a_up, lora_b_up, lora_a_down, lora_b_down):
    hid_width = HEADS * HEAD
    half_dim = HEAD // 2
    inv_freq = ROPE_BASE ** (-jnp.arange(half_dim, dtype=jnp.float32) / half_dim)
    angles = jnp.arange(SEQLEN, dtype=jnp.float32)[:, None] * inv_freq[None, :]
    cos_t = jnp.cos(angles)[:, None, :]
    sin_t = jnp.sin(angles)[:, None, :]
    causal = jnp.arange(SEQLEN)[:, None] >= jnp.arange(SEQLEN)[None, :]
    wq_flat = w_query.reshape(D, hid_width)
    wk_flat = w_key.reshape(D, hid_width)
    wv_flat = w_value.reshape(D, hid_width)
    wo_flat = w_out.reshape(hid_width, D)
    bq_flat = lora_b_query.reshape(ADAPTERS, R, hid_width)
    bk_flat = lora_b_key.reshape(ADAPTERS, R, hid_width)
    bv_flat = lora_b_value.reshape(ADAPTERS, R, hid_width)
    ao_flat = lora_a_out.reshape(ADAPTERS, hid_width, R)

    def one_sequence(seq_item):
        x_seq, adapter = seq_item
        x_f32 = x_seq.astype(jnp.float32)
        normed = (x_f32 * lax.rsqrt(jnp.mean(x_f32 * x_f32, axis=-1, keepdims=True) + EPS) * norm_gain).astype(jnp.bfloat16)
        z_query = lora_proj(normed, wq_flat, lora_a_query, bq_flat, adapter).reshape(SEQLEN, HEADS, HEAD)
        z_key = lora_proj(normed, wk_flat, lora_a_key, bk_flat, adapter).reshape(SEQLEN, HEADS, HEAD)
        z_value = lora_proj(normed, wv_flat, lora_a_value, bv_flat, adapter).reshape(SEQLEN, HEADS, HEAD)
        query_rot = rope_rotate(z_query, cos_t, sin_t).astype(jnp.bfloat16)
        key_rot = rope_rotate(z_key, cos_t, sin_t).astype(jnp.bfloat16)
        value_heads = z_value.astype(jnp.bfloat16)
        scores = jnp.einsum('qhd,khd->hqk', query_rot.astype(jnp.float32), key_rot.astype(jnp.float32)) / math.sqrt(HEAD)
        scores = jnp.where(causal[None], scores, -1e30)
        probs_bf = jax.nn.softmax(scores, axis=-1).astype(jnp.bfloat16)
        attended = jnp.einsum('hqk,khd->qhd', probs_bf.astype(jnp.float32), value_heads.astype(jnp.float32)).astype(jnp.bfloat16).reshape(SEQLEN, hid_width)
        z_out = lora_proj(attended, wo_flat, ao_flat, lora_b_out, adapter)
        gate_pre = lora_proj(normed, w_gate, lora_a_gate, lora_b_gate, adapter)
        up_pre = lora_proj(normed, w_up, lora_a_up, lora_b_up, adapter)
        mlp_mixed = (jax.nn.silu(gate_pre) * up_pre).astype(jnp.bfloat16)
        z_down = lora_proj(mlp_mixed, w_down, lora_a_down, lora_b_down, adapter)
        return (x_f32 + z_out + z_down).astype(jnp.bfloat16)

    return lax.map(one_sequence, (x, adapter_ids))
```

```python
import functools
import math

import jax
import jax.numpy as jnp
from jax import lax
from jax.experimental import pallas as pl
from jax.experimental.pallas import tpu as pltpu
from jax.sharding import PartitionSpec as P

ALPHA = 16
EPS = 1e-5
ROPE_BASE = 10000.0
VMEM_LIMIT = 60 * 1024 * 1024
LANES = 128
Q_ROWS = 256
MLP_ROWS = 512


def dot(a, b):
    return jnp.dot(a, b, preferred_element_type=jnp.float32)


def dot_t(a, b):
    return lax.dot_general(a, b, (((1,), (1,)), ((), ())), preferred_element_type=jnp.float32)


def norm_kernel(base_ref, x_ref, gain_ref, a_ref, h_ref, mid_ref):
    x_f32 = x_ref[0].astype(jnp.float32)
    h = (x_f32 * lax.rsqrt(jnp.mean(x_f32 * x_f32, axis=-1, keepdims=True) + EPS) * gain_ref[...]).astype(jnp.bfloat16)
    h_ref[0] = h
    mid_ref[0] = dot_t(h, a_ref[0]).astype(jnp.bfloat16)


def norm_call(x, base, gain, a_all, seqs):
    _, rows, width = x.shape
    n_mid = a_all.shape[1]
    blk = 512
    return pl.pallas_call(
        norm_kernel,
        grid_spec=pltpu.PrefetchScalarGridSpec(
            num_scalar_prefetch=1,
            grid=(seqs, rows // blk),
            in_specs=[
                pl.BlockSpec((1, blk, width), lambda s, r, base: (base[0] + s, r, 0)),
                pl.BlockSpec((1, width), lambda s, r, base: (0, 0)),
                pl.BlockSpec((1, n_mid, width), lambda s, r, base: (s, 0, 0)),
            ],
            out_specs=[
                pl.BlockSpec((1, blk, width), lambda s, r, base: (s, r, 0)),
                pl.BlockSpec((1, blk, n_mid), lambda s, r, base: (s, r, 0)),
            ],
        ),
        out_shape=[
            jax.ShapeDtypeStruct((seqs, rows, width), jnp.bfloat16),
            jax.ShapeDtypeStruct((seqs, rows, n_mid), jnp.bfloat16),
        ],
        compiler_params=pltpu.CompilerParams(vmem_limit_bytes=VMEM_LIMIT),
        cost_estimate=pl.CostEstimate(flops=2 * seqs * rows * width * 256, bytes_accessed=4 * seqs * rows * width, transcendentals=0),
        name="norm_mid",
    )(base, x, gain.reshape(1, width), a_all)


def attn_kernel(head, rank, scale, h_ref, mid_ref, wq_ref, wk_ref, wv_ref, b_ref, cos_ref, sin_ref, o_ref, q_s, k_s, v_s):
    rows, width = q_s.shape
    h = h_ref[0]
    lane = lax.broadcasted_iota(jnp.int32, (1, width), 1)
    first = (lane % head) < (head // 2)

    def project(i, w_ref):
        mid = mid_ref[0, :, i * rank:(i + 1) * rank]
        return dot(h, w_ref[...]) + scale * dot(mid, b_ref[0, :, i * width:(i + 1) * width])

    def rope(z):
        turned = jnp.where(first, pltpu.roll(z, width - head // 2, 1), pltpu.roll(z, head // 2, 1))
        return (z * cos_ref[...] + turned * sin_ref[...]).astype(jnp.bfloat16)

    q_s[...] = rope(project(0, wq_ref))
    k_s[...] = rope(project(1, wk_ref))
    v_s[...] = project(2, wv_ref).astype(jnp.bfloat16)

    row_i = lax.broadcasted_iota(jnp.int32, (Q_ROWS, Q_ROWS), 0)
    col_i = lax.broadcasted_iota(jnp.int32, (Q_ROWS, Q_ROWS), 1)
    causal = row_i >= col_i
    low = lax.broadcasted_iota(jnp.int32, (1, LANES), 1) < head
    factor = math.log2(math.e) / math.sqrt(head)

    for pair in range(width // LANES):
        cols = slice(pair * LANES, (pair + 1) * LANES)
        for qb in range(rows // Q_ROWS):
            begin, end = qb * Q_ROWS, (qb + 1) * Q_ROWS
            q = q_s[begin:end, cols]
            keys = k_s[:end, cols]
            vals = v_s[:end, cols]
            outs = []
            for side in range(2):
                q_one = jnp.where(low if side == 0 else ~low, q, jnp.zeros_like(q))
                s = dot_t(q_one, keys)
                s_diag = jnp.where(causal, s[:, begin:], -1e30)
                s = s_diag if qb == 0 else jnp.concatenate([s[:, :begin], s_diag], axis=1)
                peak = jnp.max(s, axis=-1, keepdims=True)
                p = jnp.exp2((s - peak) * factor)
                total = jnp.sum(p, axis=-1, keepdims=True)
                outs.append(dot((p * (1.0 / total)).astype(jnp.bfloat16), vals))
            o_ref[0, begin:end, cols] = jnp.where(low, outs[0], outs[1]).astype(jnp.bfloat16)


def attn_call(h, mid, wq, wk, wv, b_qkv, cos_t, sin_t, head, rank, scale):
    seqs, rows, width = h.shape
    cols = wq.shape[1]
    whole = lambda s: (0, 0)
    one = lambda s: (s, 0, 0)
    return pl.pallas_call(
        functools.partial(attn_kernel, head, rank, scale),
        grid=(seqs,),
        in_specs=[
            pl.BlockSpec((1, rows, width), one),
            pl.BlockSpec((1, rows, mid.shape[2]), one),
            pl.BlockSpec((width, cols), whole),
            pl.BlockSpec((width, cols), whole),
            pl.BlockSpec((width, cols), whole),
            pl.BlockSpec((1, rank, 3 * cols), one),
            pl.BlockSpec((rows, cols), whole),
            pl.BlockSpec((rows, cols), whole),
        ],
        out_specs=pl.BlockSpec((1, rows, cols), one),
        out_shape=jax.ShapeDtypeStruct((seqs, rows, cols), jnp.bfloat16),
        scratch_shapes=[pltpu.VMEM((rows, cols), jnp.bfloat16)] * 3,
        compiler_params=pltpu.CompilerParams(vmem_limit_bytes=VMEM_LIMIT),
        cost_estimate=pl.CostEstimate(flops=25_000_000_000, bytes_accessed=12 * 1024 * 1024, transcendentals=seqs * 4 * rows * rows // 2),
        name="attn",
    )(h, mid, wq, wk, wv, b_qkv, cos_t, sin_t)


def mlp_kernel(n, rank, scale, sel_ref, x_ref, h_ref, mid_ref, *rest):
    o_refs = rest[:n]
    own = rest[n:n + 4]
    sib = rest[n + 4:n + 8]
    far = rest[n + 8:n + 12]
    far_sib = rest[n + 12:n + 16]
    b_refs = rest[n + 16:n + 20]
    bo_ref, bd_ref = rest[n + 20:n + 22]
    y_ref, wo_s, wg_s, wu_s, wd_s, m_s, sems = rest[n + 22:]
    hid = wo_s.shape[1]
    ff = wg_s.shape[2]
    rows = m_s.shape[0]

    @pl.when(pl.program_id(0) == 0)
    def _load():
        copies = []
        for k, group in ((0, own), (1, sib)):
            for i, dst in enumerate((wo_s, wg_s, wu_s, wd_s)):
                copies.append(pltpu.make_async_copy(group[i], dst.at[k], sems.at[len(copies)]))
        for k, group in ((2, far), (3, far_sib)):
            for j, quarter in enumerate(group):
                place = sel_ref[j]
                offset = 0
                for dst in (wo_s, wg_s, wu_s, wd_s):
                    size = dst.shape[1] // n
                    copies.append(pltpu.make_async_copy(
                        quarter.at[pl.ds(offset, size)], dst.at[k, pl.ds(pl.multiple_of(place * size, size), size)], sems.at[len(copies)]))
                    offset += size
        for c in copies:
            c.start()
        for c in copies:
            c.wait()

    h = h_ref[0]
    mid_g = mid_ref[0, :, 3 * rank:4 * rank]
    mid_u = mid_ref[0, :, 4 * rank:5 * rank]
    heads_w = 3 * hid
    mid_d = jnp.zeros((rows, rank), jnp.float32)
    mid_o = jnp.zeros((rows, rank), jnp.float32)
    for k in range(n):
        b = b_refs[k]
        at = heads_w
        b_gate, b_up = b[0, :, at:at + ff], b[0, :, at + ff:at + 2 * ff]
        at += 2 * ff
        gate = dot(h, wg_s[k]) + scale * dot(mid_g, b_gate)
        up = dot(h, wu_s[k]) + scale * dot(mid_u, b_up)
        m = (gate * jax.nn.sigmoid(gate) * up).astype(jnp.bfloat16)
        m_s[:, k * ff:(k + 1) * ff] = m
        mid_d = mid_d + dot_t(m, b[0, :, at + hid:at + hid + ff])
        mid_o = mid_o + dot_t(o_refs[k][0], b[0, :, at:at + hid])
    total = x_ref[0].astype(jnp.float32)
    for k in range(n):
        total = total + dot(o_refs[k][0], wo_s[k])
        total = total + dot(m_s[:, k * ff:(k + 1) * ff], wd_s[k])
    total = total + scale * (dot(mid_o.astype(jnp.bfloat16), bo_ref[0]) + dot(mid_d.astype(jnp.bfloat16), bd_ref[0]))
    y_ref[...] = total.astype(jnp.bfloat16)


def mlp_call(seq, sel, x, h, mid, o_groups, own, sib, far, far_sib, b_groups, b_out, b_down, rank, scale):
    n = len(o_groups)
    _, rows, width = h.shape
    ff = own[1].shape[1]
    hid = own[0].shape[0]
    blk = MLP_ROWS
    any_spec = pl.BlockSpec(memory_space=pl.ANY)
    here = lambda r, sel: (seq, r, 0)
    seq_only = lambda r, sel: (seq, 0, 0)
    return pl.pallas_call(
        functools.partial(mlp_kernel, n, rank, scale),
        grid_spec=pltpu.PrefetchScalarGridSpec(
            num_scalar_prefetch=1,
            grid=(rows // blk,),
            in_specs=[
                pl.BlockSpec((1, blk, width), lambda r, sel: (sel[n] + seq, r, 0)),
                pl.BlockSpec((1, blk, width), here),
                pl.BlockSpec((1, blk, mid.shape[2]), here),
            ] + [pl.BlockSpec((1, blk, hid), here)] * n + [any_spec] * 16 + [
                pl.BlockSpec((1, rank, b_groups[0].shape[2]), seq_only)] * n + [
                pl.BlockSpec((1, rank, width), seq_only)] * 2,
            out_specs=pl.BlockSpec((blk, width), lambda r, sel: (r, 0)),
            scratch_shapes=[
                pltpu.VMEM((n, hid, width), jnp.bfloat16),
                pltpu.VMEM((n, width, ff), jnp.bfloat16),
                pltpu.VMEM((n, width, ff), jnp.bfloat16),
                pltpu.VMEM((n, ff, width), jnp.bfloat16),
                pltpu.VMEM((blk, n * ff), jnp.bfloat16),
                pltpu.SemaphoreType.DMA((8 + 8 * n,)),
            ],
        ),
        out_shape=jax.ShapeDtypeStruct((rows, width), jnp.bfloat16),
        compiler_params=pltpu.CompilerParams(vmem_limit_bytes=VMEM_LIMIT),
        cost_estimate=pl.CostEstimate(flops=36_000_000_000, bytes_accessed=40 * 1024 * 1024, transcendentals=rows * ff * n),
        name="mlp",
    )(sel, x, h, mid, *o_groups, *own, *sib, *far, *far_sib, *b_groups, b_out, b_down)


def blank_call(shape):
    return pl.pallas_call(
        lambda out_ref: None,
        out_specs=pl.BlockSpec(memory_space=pl.ANY),
        out_shape=jax.ShapeDtypeStruct(shape, jnp.bfloat16),
        name="blank",
    )()


def solution(mesh):
    batch_spec = P('data', None, None)
    head_cols = P(None, 'tensor', None)
    head_rows = P('tensor', None, None)
    ff_cols = P(None, 'tensor')
    ff_rows = P('tensor', None)
    last_split = P(None, None, 'tensor')
    b_heads = P(None, None, 'tensor', None)
    a_heads = P(None, 'tensor', None, None)
    in_specs = (batch_spec, P('data'), P(None), head_cols, head_cols, head_cols, head_rows, ff_cols, ff_cols, ff_rows, last_split, b_heads, last_split, b_heads, last_split, b_heads, a_heads, last_split, last_split, last_split, last_split, last_split, head_cols, last_split)
    n = mesh.shape['tensor']

    def swap(value, axis, bits):
        size = mesh.shape[axis]
        return lax.ppermute(value, axis, [(i, i ^ bits) for i in range(size)])

    def local_layer(x_blk, adapter_ids, norm_gain, w_query, w_key, w_value, w_out, w_gate, w_up, w_down, a_query, b_query, a_key, b_key, a_value, b_value, a_out, b_out, a_gate, b_gate, a_up, b_up, a_down, b_down):
        seqs, rows, width = x_blk.shape
        rank = a_out.shape[-1]
        scale = ALPHA / rank
        heads, head = w_query.shape[1:]
        hid = heads * head
        own_seqs = seqs // n
        t = lax.axis_index('tensor')
        d = lax.axis_index('data')
        order = jnp.arange(n)

        a_pack = jnp.stack([jnp.swapaxes(a[adapter_ids], 1, 2) for a in (a_query, a_key, a_value, a_gate, a_up)], axis=1)
        b_pack = jnp.concatenate(
            [b[adapter_ids].reshape(seqs, rank, -1) for b in (b_query, b_key, b_value, b_gate, b_up)]
            + [jnp.swapaxes(a_out[adapter_ids].reshape(seqs, hid, rank), 1, 2), jnp.swapaxes(a_down[adapter_ids], 1, 2),
               b_out[adapter_ids], b_down[adapter_ids]], axis=2)

        def exchange(pack):
            parts = []
            for k in range(n):
                part = lax.dynamic_slice_in_dim(pack, (t ^ k) * own_seqs, own_seqs, axis=0)
                parts.append(part if k == 0 else swap(part, 'tensor', k))
            return parts

        a_parts = exchange(a_pack)
        b_parts = exchange(b_pack)
        a_abs = jnp.stack(a_parts)[order ^ t]
        a_all = jnp.transpose(a_abs, (1, 2, 0, 3, 4)).reshape(own_seqs, -1, width)
        a_all = jnp.pad(a_all, ((0, 0), (0, LANES - a_all.shape[1]), (0, 0)))
        share = b_out.shape[-1]
        tails = jnp.stack([b[:, :, -2 * share:] for b in b_parts])[order ^ t]
        b_out_own = jnp.transpose(tails[..., :share], (1, 2, 0, 3)).reshape(own_seqs, rank, width)
        b_down_own = jnp.transpose(tails[..., share:], (1, 2, 0, 3)).reshape(own_seqs, rank, width)

        qkv = [w.reshape(width, hid) for w in (w_query, w_key, w_value)]
        own = [w_out.reshape(hid, width), w_gate, w_up, w_down]

        def quarter(w):
            size = w.shape[0] // n
            return lax.dynamic_slice_in_dim(w, d * size, size, axis=0)

        def spread(mine):
            first = swap(mine, 'tensor', 2)
            far = [first] + [swap(first, 'data', k) for k in range(1, n)]
            return far, [swap(w, 'tensor', 1) for w in far]

        qkv_own = jnp.concatenate(qkv, axis=1)
        qkv_sib = swap(qkv_own, 'tensor', 1)
        qkv_far, qkv_far_sib = spread(quarter(qkv_own))

        def assemble(parts):
            return jnp.stack(parts)[order ^ d].reshape(width, -1)

        qkv_all = [qkv_own, qkv_sib, assemble(qkv_far), assemble(qkv_far_sib)]
        sib = [swap(w, 'tensor', 1) for w in own]
        far, far_sib = spread(jnp.concatenate([quarter(w) for w in own], axis=0))

        half = head // 2
        inv_freq = ROPE_BASE ** (-jnp.arange(half, dtype=jnp.float32) / half)
        angles = jnp.arange(rows, dtype=jnp.float32)[:, None] * inv_freq[None, :]
        cos_t = jnp.tile(jnp.cos(angles), (1, 2 * heads))
        sin_t = jnp.tile(jnp.concatenate([-jnp.sin(angles), jnp.sin(angles)], axis=1), (1, heads))

        base = (t * own_seqs).astype(jnp.int32)
        h, mid = norm_call(x_blk, base.reshape(1), norm_gain, a_all, own_seqs)
        o_groups = []
        for k in range(n):
            wq, wk, wv = (qkv_all[k][:, i * hid:(i + 1) * hid] for i in range(3))
            o_groups.append(attn_call(h, mid, wq, wk, wv, b_parts[k][:, :, :3 * hid], cos_t, sin_t, head, rank, scale))

        sel = jnp.concatenate([(order ^ d).astype(jnp.int32), base.reshape(1)])
        y = blank_call((seqs, rows, width))
        for s in range(own_seqs):
            y_one = mlp_call(s, sel, x_blk, h, mid, o_groups, own, sib, far, far_sib, b_parts, b_out_own, b_down_own, rank, scale)
            y_far = swap(y_one, 'tensor', 2)
            pieces = [y_one, swap(y_one, 'tensor', 1), y_far, swap(y_far, 'tensor', 1)]
            for k in range(n):
                y = lax.dynamic_update_slice(y, pieces[k][None], ((t ^ k) * own_seqs + s, 0, 0))
        return y

    return jax.shard_map(local_layer, mesh=mesh, in_specs=in_specs, out_specs=batch_spec, check_vma=False)
```
